256 devices in a mesh: models: 2 (over y), leaf: 128 (over x, z, core).
Axes of the slice: x: 4, y: 2, z: 16, core: 2. Of those that a mesh axis runs over, the one named last changes fastest.
The devices are a block of a 4x16x16 slice.
Arguments:
- slip_rate: float32 [1048576], P(('models', 'leaf')), parts along dimension 0, may hold values from -6 to 6
- near_blocks: bfloat16 [4096, 3, 256, 256], P(('models', 'leaf')), parts along dimension 0, may hold values from -0.21875 to 0.21875
- near_index: int32 [4096, 3], P(('models', 'leaf')), parts along dimension 0, may hold values from 0 to 2047, as said below
- far_left: bfloat16 [11, 32, 1048576], P(None, None, ('models', 'leaf')), parts along dimension 2, may hold values from -1 to 1
- far_right: bfloat16 [11, 32, 1048576], P(None, None, ('models', 'leaf')), parts along dimension 2, may hold values from -6 to 6
- far_ranks: int32 [4096, 11], P(('models', 'leaf')), parts along dimension 0, may hold values from 8 to 32
Outputs:
- first_stress: float32 [1048576], P(('models', 'leaf')), parts along dimension 0
- second_stress: float32 [1048576], P(('models', 'leaf')), parts along dimension 0
The draws below stay inside these ranges and needn't reach their ends.
There are 2 independent parts, one for each index of `models`. The reference program is written for one: setup_inputs(seed, part) draws one part's arguments, and reference() takes and returns one part's arrays. A program takes and returns all parts, laid end to end along the dimension named above; each array names one. Nothing has to cross between parts.
Inputs may be any that keep to these rules, and one draw needn't show every extreme that they name: near_index[i, 0] = i; every other entry is a leaf j != i with |j - i| <= 16, and distance 16 occurs.
All inputs are finite; a program needn't handle non-finite values.
Results may differ from the reference program's by a relative error of at most 0.0045.
Values may be sent and summed in bfloat16 or wider, within the bound.
No kernel may reach another device: no remote copies, remote signals or barrier semaphores. Data moves between devices by JAX's collectives and lax.ppermute only.
A program may use at most 64 MiB of HBM per device.

```python
import math
import jax
import jax.numpy as jnp
from jax import lax

LEAF = 256
RANK = 32
NEAR = 3
LEAVES_DEV = 16
LEAVES = 2048
PATCHES = 524288
LEVELS = 11


def draw_near_index(key, part):
    base_key = jax.random.fold_in(key, 11)
    key_size, key_sign = jax.random.split(base_key)
    distance = jax.random.randint(key_size, (LEAVES, NEAR - 1), 1, LEAVES_DEV + 1)
    direction = jax.random.randint(key_sign, (LEAVES, NEAR - 1), 0, 2) * 2 - 1
    anchor = jnp.arange(LEAVES, dtype=jnp.int32)[:, None]
    target = anchor + direction * distance
    target = jnp.where((target < 0) | (target >= LEAVES), anchor - direction * distance, target)
    return jnp.concatenate([anchor, target], axis=1).astype(jnp.int32)


def set_ends(array, rng, smallest, high):
    longest = array.shape.index(max(array.shape))
    spots = []
    for shift in (0, 1):
        where = [jax.random.randint(jax.random.fold_in(rng, axis), (), 0, length) for axis, length in enumerate(array.shape)]
        where[longest] = (where[longest] + shift) % array.shape[longest]
        spots.append(tuple(where))
    return array.at[spots[0]].set(smallest).at[spots[1]].set(high)


def block_scale(rng, extent, cuts, low, high):
    def one(position, shards_of):
        steps = jax.random.uniform(jax.random.fold_in(jax.random.fold_in(rng, 6), position), (shards_of,), jnp.float32, low / len(cuts), high / len(cuts))
        return jnp.repeat(jnp.exp(steps), extent[position] // shards_of).reshape((-1,) + (1,) * (len(extent) - position - 1))

    level = one(*cuts[0])
    for cut in cuts[1:]:
        level = level * one(*cut)
    return level


def scatter_about(stream_key, dims, spread, limit, shards=(), kind=jnp.bfloat16):
    values = jax.random.normal(stream_key, dims, jnp.float32) * spread
    if len(shards) > 0:
        values = block_scale(stream_key, dims, shards, -0.22, 0.18) * values
    return jnp.clip(values, min=-limit, max=limit).astype(kind)


def setup_inputs(seed: int = 0, part: int = 0) -> dict:
    splits = jax.random.split(jax.random.key(seed), 7)
    own_keys = jax.random.split(jax.random.fold_in(splits[6], part), 7)
    return {
        "slip_rate": scatter_about(own_keys[0], (PATCHES,), 1.0, 6.0, ((0, 128),), jnp.float32),
        "near_blocks": scatter_about(own_keys[1], (LEAVES, NEAR, LEAF, LEAF), (NEAR * LEAF) ** -0.5, 0.21875, ((0, 128),)),
        "near_index": draw_near_index(jax.random.fold_in(jax.random.fold_in(splits[6], part), 71), part),
        "far_left": scatter_about(own_keys[3], (LEVELS, RANK, PATCHES), RANK ** -0.5, 1.0, ((2, 128),)),
        "far_right": scatter_about(own_keys[4], (LEVELS, RANK, PATCHES), 1.0, 6.0, ((2, 128),)),
        "far_ranks": set_ends(jax.random.randint(own_keys[5], (LEAVES, LEVELS), RANK // 4, RANK + 1), jax.random.fold_in(own_keys[5], 1), RANK // 4, RANK).astype(jnp.int32),
    }


def matvec(operand, near_blocks, near_index, far_left, far_right, far_ranks):
    leaves = near_blocks.shape[0]
    leaf_size = near_blocks.shape[2]
    levels = far_left.shape[0]
    rank_cols = far_left.shape[1]
    slip_rows = operand.reshape(leaves, leaf_size)
    picked = slip_rows[near_index].astype(jnp.float32)
    result = jnp.einsum('ikpq,ikq->ip', near_blocks.astype(jnp.float32), picked)
    rank_iota = jnp.arange(rank_cols, dtype=jnp.int32)
    rows_float = slip_rows.astype(jnp.float32)
    for level_no in range(levels):
        span_size = 2 ** level_no
        right_part = far_right[level_no].reshape(rank_cols, leaves, leaf_size).astype(jnp.float32)
        projected = jnp.einsum('rcp,cp->cr', right_part, rows_float)
        cluster_sums = projected.reshape(leaves // span_size, span_size, rank_cols).sum(axis=1)
        cluster_sums = cluster_sums * (1.0 / math.sqrt(leaf_size * span_size))
        partner = cluster_sums.reshape(-1, 2, rank_cols)[:, ::-1, :].reshape(-1, rank_cols)
        partner = jnp.repeat(partner, span_size, axis=0)
        masked = jnp.where(rank_iota[None, :] < far_ranks[:, level_no:level_no + 1], partner, 0.0)
        weights = lax.optimization_barrier(masked.astype(jnp.bfloat16))
        left_part = far_left[level_no].reshape(rank_cols, leaves, leaf_size).astype(jnp.float32)
        result = result + jnp.einsum('rcp,cr->cp', left_part, weights.astype(jnp.float32))
    return result.reshape(-1)

def reference(slip_rate, near_blocks, near_index, far_left, far_right, far_ranks):
    slip_bf = lax.optimization_barrier(slip_rate.astype(jnp.bfloat16))
    first_stress = matvec(slip_bf, near_blocks, near_index, far_left, far_right, far_ranks)
    relaxed = slip_rate + jnp.tanh(first_stress / 3.0)
    relaxed_bf = lax.optimization_barrier(relaxed.astype(jnp.bfloat16))
    second_stress = matvec(relaxed_bf, near_blocks, near_index, far_left, far_right, far_ranks)
    return (first_stress, second_stress)
```

```python
import math

import jax
import jax.numpy as jnp
from jax import lax
from jax.sharding import PartitionSpec as P


def partner_2(value, axis, stride):
    return lax.ppermute(value, axis, [(i, i ^ 1 << stride) for i in range(lax.axis_size(axis))])


def padded(block, sides, width):
    for axis, dim in sides:
        count = lax.axis_size(axis)
        forward = [(i, i + 1) for i in range(count - 1)]
        backward = [(target, source) for source, target in forward]
        low = lax.ppermute(
            lax.slice_in_dim(block, block.shape[dim] - width, None, axis=dim), axis, forward
        )
        high = lax.ppermute(lax.slice_in_dim(block, 0, width, axis=dim), axis, backward)
        block = jnp.concatenate([low, block, high], axis=dim)
    return block


def far_partners(device_sums, cross_levels):
    count = lax.axis_size("leaf")
    received = partner_2(device_sums, "leaf", 0)
    chip_sums = device_sums + received
    chips = count // 2
    me = lax.axis_index("leaf") // 2
    apart = jnp.arange(chips, dtype=jnp.int32) ^ me
    masks = [(apart >> bit_no) == 1 for bit_no in range(cross_levels - 1)]
    outgoing = sum(
        jnp.where(mask[:, None], chip_sums[bit_no + 1][None, :], 0.0)
        for bit_no, mask in enumerate(masks)
    )
    groups = [[chip * 2 + core for chip in range(chips)] for core in range(2)]
    incoming = lax.all_to_all(outgoing, "leaf", 0, 0, axis_index_groups=groups, tiled=True)
    outputs = [received[0]]
    for mask in masks:
        outputs.append(jnp.sum(jnp.where(mask[:, None], incoming, 0.0), axis=0))
    return outputs


def matvec(operand, near_blocks, near_index, far_left, far_right, far_ranks):
    local_leaves = near_blocks.shape[0]
    leaf_size = near_blocks.shape[2]
    levels = far_left.shape[0]
    rank_cols = far_left.shape[1]
    slip_rows = operand.reshape(local_leaves, leaf_size)
    extended = padded(slip_rows, (("leaf", 0),), local_leaves)
    offset = lax.axis_index("leaf") * local_leaves - local_leaves
    position = near_index - offset
    onehot = (
        position[:, :, None] == jnp.arange(3 * local_leaves, dtype=jnp.int32)[None, None, :]
    ).astype(jnp.bfloat16)
    picked = jnp.einsum("ikj,jp->ikp", onehot, extended, preferred_element_type=jnp.float32).astype(
        jnp.bfloat16
    )
    result = jnp.einsum("ikpq,ikq->ip", near_blocks, picked, preferred_element_type=jnp.float32)
    right_part = far_right.reshape(levels, rank_cols, local_leaves, leaf_size)
    projected = jnp.einsum(
        "lrcp,cp->lcr", right_part, slip_rows, preferred_element_type=jnp.float32
    )
    local_levels = local_leaves.bit_length() - 1
    cross_levels = levels - local_levels
    columns = []
    for level_no in range(local_levels):
        span_size = 2**level_no
        cluster_sums = (
            projected[level_no].reshape(local_leaves // span_size, span_size, rank_cols).sum(axis=1)
        )
        cluster_sums = cluster_sums * (1.0 / math.sqrt(leaf_size * span_size))
        partner = cluster_sums.reshape(-1, 2, rank_cols)[:, ::-1, :].reshape(-1, rank_cols)
        columns.append(jnp.repeat(partner, span_size, axis=0))
    device_sums = jnp.sum(projected[local_levels:], axis=1)
    partner_list = far_partners(device_sums, cross_levels)
    for bit_no in range(cross_levels):
        scale = 1.0 / math.sqrt(leaf_size * 2 ** (local_levels + bit_no))
        columns.append(
            jnp.broadcast_to(partner_list[bit_no][None, :] * scale, (local_leaves, rank_cols))
        )
    stacked = jnp.stack(columns)
    rank_mask = (
        jnp.arange(rank_cols, dtype=jnp.int32)[None, None, :] < jnp.transpose(far_ranks)[:, :, None]
    )
    weights = jnp.where(rank_mask, stacked, 0.0).astype(jnp.bfloat16)
    left_part = far_left.reshape(levels, rank_cols, local_leaves, leaf_size)
    result = result + jnp.einsum(
        "lrcp,lcr->cp", left_part, weights, preferred_element_type=jnp.float32
    )
    return result.reshape(-1)


def local(slip_rate, near_blocks, near_index, far_left, far_right, far_ranks):
    slip_bf = slip_rate.astype(jnp.bfloat16)
    first_stress = matvec(slip_bf, near_blocks, near_index, far_left, far_right, far_ranks)
    relaxed = slip_rate + jnp.tanh(first_stress / 3.0)
    relaxed_bf = relaxed.astype(jnp.bfloat16)
    second_stress = matvec(relaxed_bf, near_blocks, near_index, far_left, far_right, far_ranks)
    return (first_stress, second_stress)


def solution(mesh):
    in_specs = (
        P(("models", "leaf")),
        P(("models", "leaf"), None, None, None),
        P(("models", "leaf"), None),
        P(None, None, ("models", "leaf")),
        P(None, None, ("models", "leaf")),
        P(("models", "leaf"), None),
    )
    out_specs = (P(("models", "leaf")), P(("models", "leaf")))
    return jax.shard_map(local, mesh=mesh, in_specs=in_specs, out_specs=out_specs, check_vma=False)
```

```python
import math

import jax
import jax.numpy as jnp
from jax import lax
from jax.experimental import pallas as pl
from jax.experimental.pallas import tpu as pltpu
from jax.sharding import PartitionSpec as P


F32 = jnp.float32
BF16 = jnp.bfloat16
LANES = 128
NT = (((1,), (1,)), ((), ()))
VMEM_SPEC = pl.BlockSpec(memory_space=pltpu.VMEM)
ANY_SPEC = pl.BlockSpec(memory_space=pl.ANY)


def params(mib):
    return pltpu.CompilerParams(vmem_limit_bytes=mib << 20)


def sums_row(total):
    pad = -total.shape[1] % LANES
    return jnp.concatenate([total, jnp.zeros((1, pad), F32)], axis=1) if pad else total


def leaf_rows(flat):
    leaves = flat.shape[0] // 2
    return jnp.concatenate([flat[pl.ds(0, leaves, stride=2), :], flat[pl.ds(1, leaves, stride=2), :]], axis=1)


def put_rows(flat, rows):
    leaves = rows.shape[0]
    flat[pl.ds(0, leaves, stride=2), :] = rows[:, :LANES]
    flat[pl.ds(1, leaves, stride=2), :] = rows[:, LANES:]


def project_kernel(sizes, slip_hbm, far_right, sums, halo, slip, right_cross, sems):
    leaves, leaf_size, steps = sizes["leaves"], sizes["leaf_size"], sizes["steps"]
    width = leaves // steps * leaf_size
    cross = pl.ds(sizes["cross_row"], sizes["rows"] - sizes["cross_row"])
    copies = [pltpu.make_async_copy(slip_hbm, slip, sems.at[steps])]
    for c in range(steps):
        columns = pl.ds(c * width, width)
        copies.append(pltpu.make_async_copy(far_right.at[cross, columns], right_cross.at[:, columns], sems.at[c]))
    for copy in copies:
        copy.start()
    copies[0].wait()
    rows = leaf_rows(slip).astype(BF16)
    halo[...] = rows
    total = jnp.zeros((1, right_cross.shape[0]), F32)
    for leaf in range(leaves):
        if leaf % (leaves // steps) == 0:
            copies[1 + leaf // (leaves // steps)].wait()
        columns = slice(leaf * leaf_size, (leaf + 1) * leaf_size)
        total += lax.dot_general(rows[leaf : leaf + 1, :], right_cross[:, columns], NT, preferred_element_type=F32)
    sums[...] = sums_row(total)


def siblings(chip, bit_no):
    return (chip >> bit_no ^ 1) << bit_no


def spread_kernel(sizes, own, received, outgoing):
    chip = lax.axis_index("leaf") // 2
    total = own[...] + received[...]
    last = outgoing.shape[0] - 1
    outgoing[last - chip] = total[:, 0:LANES]
    for bit_no in range(sizes["cross_levels"] - 1):
        tile = sizes["rank"] * (bit_no + 1) // LANES * LANES
        start = siblings(chip, bit_no)
        for step in range(2**bit_no):
            outgoing[last - start - step] = total[:, tile : tile + LANES]


def near_part(sizes, index_copy, ranks, own, swap, cross, blocks, right, left, near_index, extended, total):
    leaves, leaf_size, near = sizes["leaves"], sizes["leaf_size"], sizes["near"]
    local_levels, rank = sizes["local_levels"], sizes["rank"]
    local_rows = local_levels * rank
    device = lax.axis_index("leaf")
    odd = device % 2
    extended[pl.ds(leaves, leaves), :] = own[...].astype(F32)
    extended[pl.ds((1 - odd) * 2 * leaves, leaves), :] = swap[...].astype(F32)
    extended[pl.ds(odd * 2 * leaves, leaves), :] = cross[...].astype(F32)
    mine = own[...]
    projected = jnp.concatenate(
        [
            lax.dot_general(
                mine[leaf : leaf + 1, :],
                right[:local_rows, leaf * leaf_size : (leaf + 1) * leaf_size],
                NT,
                preferred_element_type=F32,
            )
            for leaf in range(leaves)
        ],
        axis=0,
    )
    row = lax.broadcasted_iota(jnp.int32, projected.shape, 0)
    lane = lax.broadcasted_iota(jnp.int32, projected.shape, 1)
    level_of = lane // rank
    stacked = jnp.zeros_like(projected)
    limit = jnp.zeros_like(row)
    sums = projected
    for level_no in range(local_levels):
        span = 2**level_no
        partner = jnp.where(
            row // span % 2 == 0,
            pltpu.roll(sums, leaves - span, 0),
            pltpu.roll(sums, span, 0),
        )
        stacked = jnp.where(level_of == level_no, partner * (1.0 / math.sqrt(leaf_size * span)), stacked)
        limit = jnp.where(level_of == level_no, ranks[:, level_no : level_no + 1], limit)
        sums = sums + partner
    weights = jnp.where(lane % rank < limit, stacked, 0.0).astype(BF16)
    for leaf in range(leaves):
        columns = slice(leaf * leaf_size, (leaf + 1) * leaf_size)
        far = jnp.dot(weights, left[:local_rows, columns], preferred_element_type=F32)
        row = lax.dot_general(mine[leaf : leaf + 1, :], blocks[leaf, 0], NT, preferred_element_type=F32)
        total[leaf : leaf + 1, :] = row + far[leaf : leaf + 1, :]
    index_copy.wait()
    base = (device - 1) * leaves
    for leaf in range(leaves):
        row = total[leaf : leaf + 1, :]
        for k in range(1, near):
            picked = extended[pl.ds(near_index[k, leaf] - base, 1), :].astype(BF16)
            row += lax.dot_general(picked, blocks[leaf, k], NT, preferred_element_type=F32)
        total[leaf : leaf + 1, :] = row


def cross_weights(sizes, ranks, swapped, incoming):
    rank, leaf_size, leaves = sizes["rank"], sizes["leaf_size"], sizes["leaves"]
    local_levels, cross_levels = sizes["local_levels"], sizes["cross_levels"]
    chip = lax.axis_index("leaf") // 2
    sums = swapped[...] * (1.0 / math.sqrt(leaf_size * 2**local_levels))
    bit_of = lax.broadcasted_iota(jnp.int32, sums.shape, 1) // rank
    for bit_no in range(cross_levels - 1):
        start = siblings(chip, bit_no)
        start = incoming.shape[0] - 1 - start
        total = incoming[start]
        for step in range(1, 2**bit_no):
            total += incoming[start - step]
        total = jnp.concatenate([total] * (sums.shape[1] // LANES), axis=1)
        scale = 1.0 / math.sqrt(leaf_size * 2 ** (local_levels + 1 + bit_no))
        sums = jnp.where(bit_of == 1 + bit_no, total * scale, sums)
    width = cross_levels * rank
    lane = lax.broadcasted_iota(jnp.int32, (leaves, width), 1)
    limit = jnp.zeros((leaves, width), jnp.int32)
    for bit_no in range(cross_levels):
        level_no = local_levels + bit_no
        limit = jnp.where(lane // rank == bit_no, ranks[:, level_no : level_no + 1], limit)
    sums = jnp.broadcast_to(sums[:, :width], (leaves, width))
    return jnp.where(lane % rank < limit, sums, 0.0).astype(BF16)


def weights_kernel(sizes, ranks, swapped, incoming, weights):
    weights[...] = cross_weights(sizes, ranks, swapped, incoming)


def product(sizes, index_hbm, ranks, own, swap, cross, weights, blocks, right, left, near_index, extended, total, sem):
    leaves, leaf_size, cross_row = sizes["leaves"], sizes["leaf_size"], sizes["cross_row"]
    index_copy = pltpu.make_async_copy(index_hbm, near_index, sem)
    index_copy.start()
    near_part(sizes, index_copy, ranks, own, swap, cross, blocks, right, left, near_index, extended, total)
    for leaf in range(leaves):
        columns = slice(leaf * leaf_size, (leaf + 1) * leaf_size)
        far = jnp.dot(weights[...], left[cross_row:, columns], preferred_element_type=F32)
        total[leaf : leaf + 1, :] += far[leaf : leaf + 1, :]
    return total[...]


def middle_kernel(sizes, *refs):
    *inputs, slip, stress, sums, halo, near_index, extended, total, sem = refs
    right = inputs[7]
    leaf_size, cross_row = sizes["leaf_size"], sizes["cross_row"]
    first = product(sizes, *inputs, near_index, extended, total, sem)
    put_rows(stress, first)
    rows = (leaf_rows(slip) + jnp.tanh(first / 3.0)).astype(BF16)
    halo[...] = rows
    row = jnp.zeros((1, right.shape[0] - cross_row), F32)
    for leaf in range(sizes["leaves"]):
        columns = slice(leaf * leaf_size, (leaf + 1) * leaf_size)
        row += lax.dot_general(rows[leaf : leaf + 1, :], right[cross_row:, columns], NT, preferred_element_type=F32)
    sums[...] = sums_row(row)


def last_kernel(sizes, *refs):
    *inputs, first, first_stress, stress, near_index, extended, total, sem = refs
    first_stress[...] = first[...]
    put_rows(stress, product(sizes, *inputs, near_index, extended, total, sem))


def vmem(*arrays):
    return tuple(pltpu.with_memory_space_constraint(a, pltpu.VMEM) for a in arrays)


def hbm(*arrays):
    return tuple(pltpu.with_memory_space_constraint(a, pltpu.HBM) for a in arrays)


def call(kernel, out_shape, in_specs, mib, scratch=(), cost=None):
    outs = out_shape if isinstance(out_shape, tuple) else (out_shape,)
    specs = tuple(VMEM_SPEC for _ in outs)
    return pl.pallas_call(
        kernel,
        out_shape=out_shape,
        in_specs=in_specs,
        out_specs=specs if isinstance(out_shape, tuple) else specs[0],
        scratch_shapes=scratch,
        compiler_params=params(mib),
        cost_estimate=cost,
    )


def local(slip_rate, near_blocks, near_index, far_left, far_right, far_ranks):
    leaves, near, leaf_size, _ = near_blocks.shape
    levels, rank, patches = far_left.shape
    local_levels = leaves.bit_length() - 1
    devices = lax.axis_size("leaf")
    chips = devices // 2
    local_rows = local_levels * rank
    cross_rows = levels * rank - local_rows
    sizes = dict(
        leaves=leaves, near=near, leaf_size=leaf_size, rank=rank, rows=levels * rank, steps=8,
        local_levels=local_levels, cross_levels=levels - local_levels, cross_row=local_rows,
    )
    slip = slip_rate.reshape(-1, LANES)
    left = far_left.reshape(levels * rank, patches)
    right = far_right.reshape(levels * rank, patches)
    near_index = near_index.T
    sums_shape = jax.ShapeDtypeStruct((1, cross_rows + -cross_rows % LANES), F32)
    halo_shape = jax.ShapeDtypeStruct((leaves, leaf_size), BF16)
    stress_shape = jax.ShapeDtypeStruct(slip.shape, F32)
    swap = [(i, i ^ 1) for i in range(devices)]
    across = [(i, (i + 1) % devices) for i in range(1, devices, 2)]
    across += [(j, i) for i, j in across]
    groups = [[chip * 2 + core for chip in reversed(range(chips))] for core in range(2)]
    scratch = [
        pltpu.SMEM(near_index.shape, jnp.int32),
        pltpu.VMEM((3 * leaves, leaf_size), F32),
        pltpu.VMEM((leaves, leaf_size), F32),
        pltpu.SemaphoreType.DMA,
    ]
    kept = vmem(near_blocks, right, left)
    product_specs = [ANY_SPEC] + [VMEM_SPEC] * 8

    wait = pl.CostEstimate(flops=10**10, transcendentals=0, bytes_accessed=0)

    def exchange(sums, halo):
        halo_cross = lax.ppermute(halo, "leaf", across)
        halo_swap = lax.ppermute(halo, "leaf", swap)
        swapped = lax.ppermute(sums, "leaf", swap)
        outgoing = call(
            lambda *refs: spread_kernel(sizes, *refs),
            jax.ShapeDtypeStruct((chips, 1, LANES), F32),
            [VMEM_SPEC] * 2, 1, cost=wait,
        )(sums, swapped)
        incoming = lax.all_to_all(outgoing, "leaf", 0, 0, axis_index_groups=groups, tiled=True)
        weights = call(
            lambda *refs: weights_kernel(sizes, *refs),
            jax.ShapeDtypeStruct((leaves, cross_rows), BF16),
            [VMEM_SPEC] * 3, 1,
        )(far_ranks, swapped, incoming)
        return near_index, far_ranks, halo, halo_swap, halo_cross, weights, *kept

    sums, halo = call(
        lambda *refs: project_kernel(sizes, *refs),
        (sums_shape, halo_shape),
        [ANY_SPEC, ANY_SPEC], 4,
        [
            pltpu.VMEM(slip.shape, F32),
            pltpu.VMEM((cross_rows, patches), BF16),
            pltpu.SemaphoreType.DMA((sizes["steps"] + 1,)),
        ],
    )(*hbm(slip, right))
    inputs = exchange(sums, halo)
    first_stress, sums, halo = call(
        lambda *refs: middle_kernel(sizes, *refs),
        (pltpu.VMEM(slip.shape, F32), sums_shape, halo_shape),
        product_specs + [VMEM_SPEC], 4, scratch,
    )(*inputs, *vmem(slip))
    inputs = exchange(sums, halo)
    first_stress, second_stress = call(
        lambda *refs: last_kernel(sizes, *refs), (stress_shape, stress_shape), product_specs + [VMEM_SPEC], 4,
        scratch,
    )(*inputs, *vmem(first_stress))
    return (first_stress.reshape(-1), second_stress.reshape(-1))


def solution(mesh):
    in_specs = (
        P(("models", "leaf")),
        P(("models", "leaf"), None, None, None),
        P(("models", "leaf"), None),
        P(None, None, ("models", "leaf")),
        P(None, None, ("models", "leaf")),
        P(("models", "leaf"), None),
    )
    out_specs = (P(("models", "leaf")), P(("models", "leaf")))
    return jax.shard_map(local, mesh=mesh, in_specs=in_specs, out_specs=out_specs, check_vma=False)
```

```python
import math

import jax
import jax.numpy as jnp
from jax import lax
from jax.experimental import pallas as pl
from jax.experimental.pallas import tpu as pltpu
from jax.sharding import PartitionSpec as P


F32 = jnp.float32
BF16 = jnp.bfloat16
LANES = 128
SUBLANES = 8
RING = 32
NT = (((1,), (1,)), ((), ()))
TN = (((0,), (0,)), ((), ()))
VMEM_SPEC = pl.BlockSpec(memory_space=pltpu.VMEM)
ANY_SPEC = pl.BlockSpec(memory_space=pl.ANY)


def early(devices):
    return lax.axis_index("leaf") % RING < devices


def ahead(sizes):
    return jnp.logical_and(early(sizes["ahead"]), lax.axis_index("models") + lax.axis_index("leaf") > 0)


def sums_row(total):
    total = jnp.sum(total, axis=0, keepdims=True)
    pad = -total.shape[1] % LANES
    return jnp.concatenate([total, jnp.zeros((1, pad), F32)], axis=1) if pad else total


def rows_of(ref, leaves):
    if ref.shape[1] != LANES:
        return ref[:leaves, :]
    return jnp.concatenate([ref[pl.ds(0, leaves, stride=2), :], ref[pl.ds(1, leaves, stride=2), :]], axis=1)


def put_rows(flat, rows):
    leaves = rows.shape[0]
    flat[pl.ds(0, leaves, stride=2), :] = rows[:, :LANES]
    flat[pl.ds(1, leaves, stride=2), :] = rows[:, LANES:]


def columns_of(sizes, leaf):
    return slice(leaf * sizes["leaf_size"], (leaf + 1) * sizes["leaf_size"])


def pick_row(leaf, array):
    row = lax.broadcasted_iota(jnp.int32, array.shape, 0)
    return jnp.where(row == leaf, array, 0.0)


def project_leaf(rows, factor, leaf):
    return pick_row(leaf, lax.dot_general(rows, factor, NT, preferred_element_type=F32))


def project(sizes, slip_hbm, far_right, sums, own, slip, right_cross, sems):
    leaves, steps = sizes["leaves"], sizes["steps"]
    step = leaves // steps
    cross = pl.ds(sizes["cross_row"], sizes["cross_rows"])
    copies = [pltpu.make_async_copy(slip_hbm, slip, sems.at[steps])]
    for c in range(steps):
        columns = pl.ds(c * step * sizes["leaf_size"], step * sizes["leaf_size"])
        copies.append(pltpu.make_async_copy(far_right.at[cross, columns], right_cross.at[:, columns], sems.at[c]))
    for copy in copies:
        copy.start()
    copies[0].wait()
    own[...] = rows_of(slip, leaves)
    rows = own[...].astype(BF16)
    total = jnp.zeros((leaves, right_cross.shape[0]), F32)
    for leaf in range(leaves):
        if leaf % step == 0:
            copies[1 + leaf // step].wait()
        total += project_leaf(rows, right_cross[:, columns_of(sizes, leaf)], leaf)
    sums[...] = sums_row(total)


def project_early_kernel(sizes, *refs):
    @pl.when(early(RING // 2))
    def _():
        project(sizes, *refs)


def project_late_kernel(sizes, slip_hbm, far_right, early_sums, early_own, sums, own, *scratch):
    done = early(RING // 2)

    @pl.when(done)
    def _():
        sums[...] = early_sums[...]
        own[...] = early_own[...]

    @pl.when(jnp.logical_not(done))
    def _():
        project(sizes, slip_hbm, far_right, sums, own, *scratch)


def place_of(chip, chips):
    return (chips - 1 - chips // 4 - chip) & (chips - 1)


def siblings(chip, chips, bit_no):
    start = (chip >> bit_no ^ 1) << bit_no
    return [place_of(start + step, chips) for step in range(2**bit_no)]


def lane_of(sizes, bit_no):
    return sizes["rank"] * (bit_no + 1)


def spread_kernel(sizes, own, _, outgoing):
    chip = lax.axis_index("leaf") // 2
    chips = outgoing.shape[0]
    total = own[...]
    outgoing[place_of(chip, chips)] = total[:, :LANES]
    for bit_no in range(sizes["cross_levels"] - 1):
        tile = lane_of(sizes, bit_no) // LANES * LANES
        for place in siblings(chip, chips, bit_no):
            outgoing[place] = total[:, tile : tile + LANES]


def gather_kernel(sizes, own, incoming, rows, packet):
    leaves = sizes["leaves"]
    chip = lax.axis_index("leaf") // 2
    total = own[...]
    bit_of = lax.broadcasted_iota(jnp.int32, total.shape, 1) // sizes["rank"]
    for bit_no in range(sizes["cross_levels"] - 1):
        part = sum(incoming[place] for place in siblings(chip, incoming.shape[0], bit_no))
        total = jnp.where(bit_of == 1 + bit_no, jnp.concatenate([part] * (total.shape[1] // LANES), axis=1), total)
    packet[:leaves, :] = rows_of(rows, leaves).astype(F32)
    packet[leaves:, :] = jnp.broadcast_to(total, (SUBLANES, total.shape[1]))


def far_scales(sizes, ranks, first_level, levels):
    rank, leaf_size = sizes["rank"], sizes["leaf_size"]
    shape = (sizes["leaves"], levels * rank)
    lane = lax.broadcasted_iota(jnp.int32, shape, 1)
    limit, scale = jnp.zeros(shape, jnp.int32), jnp.zeros(shape, F32)
    for number in range(levels):
        level = first_level + number
        here = lane // rank == number
        limit = jnp.where(here, ranks[:, level : level + 1], limit)
        scale = jnp.where(here, 1.0 / math.sqrt(leaf_size * 2**level), scale)
    return jnp.where(lane % rank < limit, scale, 0.0)


def own_part(sizes, ranks, own, blocks, right, left):
    leaves, local_levels, rank = sizes["leaves"], sizes["local_levels"], sizes["rank"]
    local_rows = local_levels * rank
    rows = rows_of(own, leaves).astype(BF16)
    sums = jnp.zeros((leaves, local_rows), F32)
    for leaf in range(leaves):
        sums += project_leaf(rows, right[:local_rows, columns_of(sizes, leaf)], leaf)
    total = jnp.zeros((leaves, sizes["leaf_size"]), F32)
    for leaf in range(leaves):
        total += project_leaf(rows, blocks[leaf, 0], leaf)
    row = lax.broadcasted_iota(jnp.int32, sums.shape, 0)
    level_of = lax.broadcasted_iota(jnp.int32, sums.shape, 1) // rank
    stacked = sums
    for level in range(local_levels):
        span = 2**level
        low = row // span % 2 == 0
        partner = jnp.where(low, pltpu.roll(sums, leaves - span, 0), pltpu.roll(sums, span, 0))
        stacked = jnp.where(level_of == level, partner, stacked)
        sums = sums + partner
    weights = (stacked * far_scales(sizes, ranks, 0, local_levels)).astype(BF16)
    for leaf in range(leaves):
        total += pick_row(
            leaf, jnp.dot(weights, left[:local_rows, columns_of(sizes, leaf)], preferred_element_type=F32)
        )
    return total


def other_rows(sizes, near_index, own, swap, cross):
    leaves, near = sizes["leaves"], sizes["near"]
    device = lax.axis_index("leaf")
    odd = jnp.full((leaves, sizes["leaf_size"]), device % 2) == 1
    own, swap, cross = (rows_of(ref, leaves).astype(BF16).astype(F32) for ref in (own, swap, cross))
    extended = jnp.concatenate([jnp.where(odd, swap, cross), own, jnp.where(odd, cross, swap)], axis=0).astype(BF16)
    place = near_index[...] - (device - 1) * leaves
    row = lax.broadcasted_iota(jnp.int32, (3 * leaves, leaves), 0)
    picked = jnp.concatenate([jnp.where(row == place[k : k + 1, :], 1.0, 0.0) for k in range(1, near)], axis=1)
    rows = lax.dot_general(picked.astype(BF16), extended, TN, preferred_element_type=F32).astype(BF16)
    return [rows[k * leaves : (k + 1) * leaves, :] for k in range(near - 1)]


def own_ahead_kernel(
    sizes, ranks_hbm, own, blocks_hbm, right_hbm, left_hbm, partial, ranks, blocks, right, left, sems
):
    @pl.when(ahead(sizes))
    def _():
        local_rows = pl.ds(0, right.shape[0])
        copies = [
            pltpu.make_async_copy(right_hbm.at[local_rows], right, sems.at[0]),
            pltpu.make_async_copy(left_hbm.at[local_rows], left, sems.at[1]),
            pltpu.make_async_copy(blocks_hbm.at[:, pl.ds(0, 1)], blocks, sems.at[2]),
            pltpu.make_async_copy(ranks_hbm, ranks, sems.at[3]),
        ]
        for copy in copies:
            copy.start()
        for copy in copies:
            copy.wait()
        partial[...] = own_part(sizes, ranks, own, blocks, right, left)


def own_kernel(sizes, ranks, own, blocks, right, left, before, _, partial, *scales):
    done = ahead(sizes)
    if scales:
        scales[0][...] = far_scales(sizes, ranks, sizes["local_levels"], sizes["cross_levels"])

    @pl.when(done)
    def _():
        partial[...] = before[...]

    @pl.when(jnp.logical_not(done))
    def _():
        partial[...] = own_part(sizes, ranks, own, blocks, right, left)


def product(sizes, near_index, partial, scales, own, packet, swapped, cross, blocks, left):
    leaves, cross_row, width = sizes["leaves"], sizes["cross_row"], sizes["cross_rows"]
    picked = other_rows(sizes, near_index, own, swapped, cross)
    sums, others = packet[leaves : leaves + 1, :], swapped[leaves : leaves + 1, :]
    lane = lax.broadcasted_iota(jnp.int32, sums.shape, 1)
    sums = others + jnp.where(lane < sizes["rank"], 0.0, sums)
    weights = (jnp.broadcast_to(sums[:, :width], (leaves, width)) * scales[...]).astype(BF16)
    result = partial[...]
    for leaf in range(leaves):
        result += pick_row(leaf, jnp.dot(weights, left[cross_row:, columns_of(sizes, leaf)], preferred_element_type=F32))
    for k, rows in enumerate(picked):
        for leaf in range(leaves):
            result += project_leaf(rows, blocks[leaf, 1 + k], leaf)
    return result


def middle_kernel(sizes, *refs):
    *inputs, slip, stress, halo = refs
    first = product(sizes, *inputs)
    halo[...] = (rows_of(slip, sizes["leaves"]) + jnp.tanh(first / 3.0)).astype(BF16)
    put_rows(stress, first)


def project_again(sizes, own, right, sums):
    total = jnp.zeros((sizes["leaves"], sizes["cross_rows"]), F32)
    for leaf in range(sizes["leaves"]):
        total += project_leaf(own[...], right[sizes["cross_row"] :, columns_of(sizes, leaf)], leaf)
    sums[...] = sums_row(total)


def ahead_again_kernel(sizes, ranks, own, blocks, right, left, partial, sums):
    @pl.when(early(sizes["ahead"]))
    def _():
        project_again(sizes, own, right, sums)

    @pl.when(ahead(sizes))
    def _():
        partial[...] = own_part(sizes, ranks, own, blocks, right, left)


def project_again_kernel(sizes, own, right, before, sums):
    done = early(sizes["ahead"])

    @pl.when(done)
    def _():
        sums[...] = before[...]

    @pl.when(jnp.logical_not(done))
    def _():
        project_again(sizes, own, right, sums)


def last_kernel(sizes, *refs):
    *inputs, first, first_stress, stress = refs
    first_stress[...] = first[...]
    put_rows(stress, product(sizes, *inputs))


def vmem(*arrays):
    return tuple(pltpu.with_memory_space_constraint(a, pltpu.VMEM) for a in arrays)


def hbm(*arrays):
    return tuple(pltpu.with_memory_space_constraint(a, pltpu.HBM) for a in arrays)


def local(slip_rate, near_blocks, near_index, far_left, far_right, far_ranks):
    leaves, near, leaf_size, _ = near_blocks.shape
    levels, rank, patches = far_left.shape
    local_levels = leaves.bit_length() - 1
    devices = lax.axis_size("leaf")
    chips = devices // 2
    local_rows = local_levels * rank
    cross_rows = levels * rank - local_rows
    sizes = dict(
        leaves=leaves, near=near, leaf_size=leaf_size, rank=rank, local_levels=local_levels,
        cross_levels=levels - local_levels, cross_row=local_rows, cross_rows=cross_rows, steps=2, ahead=6,
    )
    slip = slip_rate.reshape(-1, LANES)
    left = far_left.reshape(levels * rank, patches)
    right = far_right.reshape(levels * rank, patches)
    near_index = near_index.T
    shape = jax.ShapeDtypeStruct
    sums_shape = shape((1, cross_rows + -cross_rows % LANES), F32)
    partial_shape = shape((leaves, leaf_size), F32)
    stress_shape = shape(slip.shape, F32)
    swap = [(i, i ^ 1) for i in range(devices)]
    across = [(i, (i + 1) % devices) for i in range(1, devices, 2)]
    across += [(j, i) for i, j in across]
    order = sorted(range(chips), key=lambda chip: place_of(chip, chips))
    groups = [[chip * 2 + core for chip in order] for core in range(2)]

    def call(kernel, out_shape, specs, operands, mib=4, scratch=(), cost=None):
        outs = out_shape if isinstance(out_shape, tuple) else (out_shape,)
        return pl.pallas_call(
            lambda *refs: kernel(sizes, *refs),
            out_shape=out_shape,
            in_specs=specs,
            out_specs=tuple(VMEM_SPEC for _ in outs) if isinstance(out_shape, tuple) else VMEM_SPEC,
            scratch_shapes=scratch,
            compiler_params=pltpu.CompilerParams(vmem_limit_bytes=mib << 20),
            cost_estimate=cost,
        )(*operands)

    def permute(array, pairs):
        return lax.ppermute(array, "leaf", pairs)

    wait = pl.CostEstimate(flops=10**10, transcendentals=0, bytes_accessed=0)

    def exchange(sums, before, rows):
        outgoing = call(
            spread_kernel, shape((chips, 1, LANES), F32), [VMEM_SPEC, ANY_SPEC], (sums, before), 1, cost=wait
        )
        incoming = lax.all_to_all(outgoing, "leaf", 0, 0, axis_index_groups=groups, tiled=True)
        packet = call(
            gather_kernel, shape((leaves + SUBLANES, leaf_size), F32), [VMEM_SPEC] * 3, (sums, incoming, rows), 1
        )
        return packet, permute(packet, swap)

    kept = vmem(near_blocks, right, left)
    own_specs = [VMEM_SPEC] * 6 + [ANY_SPEC]
    product_specs = [VMEM_SPEC] * 9

    halo_cross = permute(slip_rate, across).reshape(-1, LANES)
    project_scratch = [
        pltpu.VMEM(slip.shape, F32),
        pltpu.VMEM((cross_rows, patches), BF16),
        pltpu.SemaphoreType.DMA((sizes["steps"] + 1,)),
    ]
    sums, own = call(
        project_early_kernel, (sums_shape, partial_shape), [ANY_SPEC] * 2, hbm(slip, right),
        scratch=project_scratch,
    )
    before = call(
        own_ahead_kernel, partial_shape, [ANY_SPEC, VMEM_SPEC] + [ANY_SPEC] * 3,
        (*hbm(far_ranks), own, *hbm(near_blocks, right, left)), 8,
        [
            pltpu.VMEM(far_ranks.shape, jnp.int32),
            pltpu.VMEM((leaves, 1, leaf_size, leaf_size), BF16),
            pltpu.VMEM((local_rows, patches), BF16),
            pltpu.VMEM((local_rows, patches), BF16),
            pltpu.SemaphoreType.DMA((4,)),
        ],
    )
    sums, own = call(
        project_late_kernel, (sums_shape, partial_shape), [ANY_SPEC] * 2 + [VMEM_SPEC] * 2,
        (*hbm(slip, right), sums, own),
        scratch=project_scratch,
    )
    packet, swapped = exchange(sums, before, own)
    partial, scales = call(
        own_kernel, (partial_shape, shape((leaves, cross_rows), F32)), own_specs,
        (far_ranks, own, *kept, before, packet),
    )
    first_stress, halo = call(
        middle_kernel, (pltpu.VMEM(slip.shape, F32), shape((leaves, leaf_size), BF16)), product_specs + [VMEM_SPEC],
        (near_index, partial, scales, own, packet, swapped, halo_cross, kept[0], kept[2], own),
    )
    halo_cross = permute(halo, across)
    before, sums = call(ahead_again_kernel, (partial_shape, sums_shape), [VMEM_SPEC] * 5, (far_ranks, halo, *kept))
    sums = call(project_again_kernel, sums_shape, [VMEM_SPEC] * 3, (halo, kept[1], sums))
    packet, swapped = exchange(sums, before, halo)
    partial = call(own_kernel, partial_shape, own_specs, (far_ranks, halo, *kept, before, packet))
    first_stress, second_stress = call(
        last_kernel, (stress_shape, stress_shape), product_specs + [VMEM_SPEC],
        (near_index, partial, scales, halo, packet, swapped, halo_cross, kept[0], kept[2], *vmem(first_stress)),
    )
    return (first_stress.reshape(-1), second_stress.reshape(-1))


def solution(mesh):
    in_specs = (
        P(("models", "leaf")),
        P(("models", "leaf"), None, None, None),
        P(("models", "leaf"), None),
        P(None, None, ("models", "leaf")),
        P(None, None, ("models", "leaf")),
        P(("models", "leaf"), None),
    )
    out_specs = (P(("models", "leaf")), P(("models", "leaf")))
    return jax.shard_map(local, mesh=mesh, in_specs=in_specs, out_specs=out_specs, check_vma=False)
```

```python
import math

import jax
import jax.numpy as jnp
from jax import lax
from jax.experimental import pallas as pl
from jax.experimental.pallas import tpu as pltpu
from jax.sharding import PartitionSpec as P


F32 = jnp.float32
BF16 = jnp.bfloat16
LANES = 128
SUBLANES = 8
RING = 32
NT = (((1,), (1,)), ((), ()))
TN = (((0,), (0,)), ((), ()))
VMEM_SPEC = pl.BlockSpec(memory_space=pltpu.VMEM)
ANY_SPEC = pl.BlockSpec(memory_space=pl.ANY)


def early(devices):
    return lax.axis_index("leaf") % RING < devices


def ahead(sizes):
    return jnp.logical_and(early(sizes["ahead"]), lax.axis_index("models") + lax.axis_index("leaf") > 0)


def sums_row(total):
    total = jnp.sum(total, axis=0, keepdims=True)
    pad = -total.shape[1] % LANES
    return jnp.concatenate([total, jnp.zeros((1, pad), F32)], axis=1) if pad else total


def rows_of(ref, leaves):
    if ref.shape[1] != LANES:
        return ref[:leaves, :]
    return jnp.concatenate([ref[pl.ds(0, leaves, stride=2), :], ref[pl.ds(1, leaves, stride=2), :]], axis=1)


def put_rows(flat, rows):
    leaves = rows.shape[0]
    flat[pl.ds(0, leaves, stride=2), :] = rows[:, :LANES]
    flat[pl.ds(1, leaves, stride=2), :] = rows[:, LANES:]


def columns_of(sizes, leaf):
    return slice(leaf * sizes["leaf_size"], (leaf + 1) * sizes["leaf_size"])


def pick_row(leaf, array):
    row = lax.broadcasted_iota(jnp.int32, array.shape, 0)
    return jnp.where(row == leaf, array, 0.0)


def project_leaf(rows, factor, leaf):
    return pick_row(leaf, lax.dot_general(rows, factor, NT, preferred_element_type=F32))


def project(sizes, slip_hbm, far_right, sums, own, slip, right_cross, sems):
    leaves, steps = sizes["leaves"], sizes["steps"]
    step = leaves // steps
    cross = pl.ds(sizes["cross_row"], sizes["cross_rows"])
    copies = [pltpu.make_async_copy(slip_hbm, slip, sems.at[steps])]
    for c in range(steps):
        columns = pl.ds(c * step * sizes["leaf_size"], step * sizes["leaf_size"])
        copies.append(pltpu.make_async_copy(far_right.at[cross, columns], right_cross.at[:, columns], sems.at[c]))
    for copy in copies:
        copy.start()
    copies[0].wait()
    own[...] = rows_of(slip, leaves)
    rows = own[...].astype(BF16)
    total = jnp.zeros((leaves, right_cross.shape[0]), F32)
    for leaf in range(leaves):
        if leaf % step == 0:
            copies[1 + leaf // step].wait()
        total += project_leaf(rows, right_cross[:, columns_of(sizes, leaf)], leaf)
    sums[...] = sums_row(total)


def project_early_kernel(sizes, *refs):
    @pl.when(early(RING // 2))
    def _():
        project(sizes, *refs)


def project_late_kernel(sizes, slip_hbm, far_right, early_sums, early_own, sums, own, *scratch):
    done = early(RING // 2)

    @pl.when(done)
    def _():
        sums[...] = early_sums[...]
        own[...] = early_own[...]

    @pl.when(jnp.logical_not(done))
    def _():
        project(sizes, slip_hbm, far_right, sums, own, *scratch)


def place_of(chip, chips):
    return (chips - 1 - chips // 4 - chip) & (chips - 1)


def siblings(chip, chips, bit_no):
    start = (chip >> bit_no ^ 1) << bit_no
    return [place_of(start + step, chips) for step in range(2**bit_no)]


def lane_of(sizes, bit_no):
    return sizes["rank"] * (bit_no + 1)


def spread_kernel(sizes, own, _, outgoing):
    chip = lax.axis_index("leaf") // 2
    chips = outgoing.shape[0]
    total = own[...]
    outgoing[place_of(chip, chips)] = total[:, :LANES]
    for bit_no in range(sizes["cross_levels"] - 1):
        tile = lane_of(sizes, bit_no) // LANES * LANES
        for place in siblings(chip, chips, bit_no):
            outgoing[place] = total[:, tile : tile + LANES]


def gather_kernel(sizes, own, incoming, *refs):
    leaves = sizes["leaves"]
    chip = lax.axis_index("leaf") // 2
    total = own[...]
    bit_of = lax.broadcasted_iota(jnp.int32, total.shape, 1) // sizes["rank"]
    for bit_no in range(sizes["cross_levels"] - 1):
        part = sum(incoming[place] for place in siblings(chip, incoming.shape[0], bit_no))
        total = jnp.where(bit_of == 1 + bit_no, jnp.concatenate([part] * (total.shape[1] // LANES), axis=1), total)
    *rows, packet = refs
    if rows:
        packet[:leaves, :] = rows_of(rows[0], leaves).astype(F32)
        total = jnp.broadcast_to(total, (SUBLANES, total.shape[1]))
    packet[packet.shape[0] - total.shape[0] :, :] = total


def far_scales(sizes, ranks, first_level, levels):
    rank, leaf_size = sizes["rank"], sizes["leaf_size"]
    shape = (sizes["leaves"], levels * rank)
    lane = lax.broadcasted_iota(jnp.int32, shape, 1)
    limit, scale = jnp.zeros(shape, jnp.int32), jnp.zeros(shape, F32)
    for number in range(levels):
        level = first_level + number
        here = lane // rank == number
        limit = jnp.where(here, ranks[:, level : level + 1], limit)
        scale = jnp.where(here, 1.0 / math.sqrt(leaf_size * 2**level), scale)
    return jnp.where(lane % rank < limit, scale, 0.0)


def own_part(sizes, ranks, own, blocks, right, left):
    leaves, local_levels, rank = sizes["leaves"], sizes["local_levels"], sizes["rank"]
    local_rows = local_levels * rank
    rows = rows_of(own, leaves).astype(BF16)
    sums = jnp.zeros((leaves, local_rows), F32)
    for leaf in range(leaves):
        sums += project_leaf(rows, right[:local_rows, columns_of(sizes, leaf)], leaf)
    total = jnp.zeros((leaves, sizes["leaf_size"]), F32)
    for leaf in range(leaves):
        total += project_leaf(rows, blocks[leaf, 0], leaf)
    row = lax.broadcasted_iota(jnp.int32, sums.shape, 0)
    level_of = lax.broadcasted_iota(jnp.int32, sums.shape, 1) // rank
    stacked = sums
    for level in range(local_levels):
        span = 2**level
        low = row // span % 2 == 0
        partner = jnp.where(low, pltpu.roll(sums, leaves - span, 0), pltpu.roll(sums, span, 0))
        stacked = jnp.where(level_of == level, partner, stacked)
        sums = sums + partner
    weights = (stacked * far_scales(sizes, ranks, 0, local_levels)).astype(BF16)
    for leaf in range(leaves):
        total += pick_row(
            leaf, jnp.dot(weights, left[:local_rows, columns_of(sizes, leaf)], preferred_element_type=F32)
        )
    return total


def other_rows(sizes, near_index, own, swap, cross):
    leaves, near = sizes["leaves"], sizes["near"]
    device = lax.axis_index("leaf")
    odd = jnp.full((leaves, sizes["leaf_size"]), device % 2) == 1
    own, swap, cross = (rows_of(ref, leaves).astype(BF16).astype(F32) for ref in (own, swap, cross))
    extended = jnp.concatenate([jnp.where(odd, swap, cross), own, jnp.where(odd, cross, swap)], axis=0).astype(BF16)
    place = near_index[...] - (device - 1) * leaves
    row = lax.broadcasted_iota(jnp.int32, (3 * leaves, leaves), 0)
    picked = jnp.concatenate([jnp.where(row == place[k : k + 1, :], 1.0, 0.0) for k in range(1, near)], axis=1)
    rows = lax.dot_general(picked.astype(BF16), extended, TN, preferred_element_type=F32).astype(BF16)
    return [rows[k * leaves : (k + 1) * leaves, :] for k in range(near - 1)]


def own_ahead_kernel(
    sizes, ranks_hbm, own, blocks_hbm, right_hbm, left_hbm, partial, ranks, blocks, right, left, sems
):
    @pl.when(ahead(sizes))
    def _():
        local_rows = pl.ds(0, right.shape[0])
        copies = [
            pltpu.make_async_copy(right_hbm.at[local_rows], right, sems.at[0]),
            pltpu.make_async_copy(left_hbm.at[local_rows], left, sems.at[1]),
            pltpu.make_async_copy(blocks_hbm.at[:, pl.ds(0, 1)], blocks, sems.at[2]),
            pltpu.make_async_copy(ranks_hbm, ranks, sems.at[3]),
        ]
        for copy in copies:
            copy.start()
        for copy in copies:
            copy.wait()
        partial[...] = own_part(sizes, ranks, own, blocks, right, left)


def second_core():
    return lax.axis_index("leaf") % 2 == 1


def own_or_before(sizes, ranks, own, blocks, right, left, before, partial):
    done = ahead(sizes)

    @pl.when(done)
    def _():
        partial[...] = before[...]

    @pl.when(jnp.logical_not(done))
    def _():
        partial[...] = own_part(sizes, ranks, own, blocks, right, left)


def own_second_kernel(sizes, ranks, own, blocks, right, left, before, packet, partial, packet_out):
    packet_out[...] = packet[...]

    @pl.when(second_core())
    def _():
        own_or_before(sizes, ranks, own, blocks, right, left, before, partial)


def own_first_kernel(sizes, ranks, own, blocks, right, left, before, second, _, partial, scales):
    scales[...] = far_scales(sizes, ranks, sizes["local_levels"], sizes["cross_levels"])

    @pl.when(second_core())
    def _():
        partial[...] = second[...]

    @pl.when(jnp.logical_not(second_core()))
    def _():
        own_or_before(sizes, ranks, own, blocks, right, left, before, partial)


def other_part(sizes, picked, blocks):
    total = jnp.zeros((sizes["leaves"], sizes["leaf_size"]), F32)
    for k, rows in enumerate(picked):
        for leaf in range(sizes["leaves"]):
            total += project_leaf(rows, blocks[leaf, 1 + k], leaf)
    return total


def near_kernel(sizes, near_index, ranks, own, swap, cross, blocks, right, left, before, _, partial):
    picked = other_rows(sizes, near_index, own, swap, cross)
    own_or_before(sizes, ranks, own, blocks, right, left, before, partial)
    partial[...] += other_part(sizes, picked, blocks)


def cross_part(sizes, scales, packet, swapped, left):
    leaves, cross_row, width = sizes["leaves"], sizes["cross_row"], sizes["cross_rows"]
    sums, others = packet[packet.shape[0] - 1 :, :], swapped[swapped.shape[0] - 1 :, :]
    lane = lax.broadcasted_iota(jnp.int32, sums.shape, 1)
    sums = others + jnp.where(lane < sizes["rank"], 0.0, sums)
    weights = (jnp.broadcast_to(sums[:, :width], (leaves, width)) * scales[...]).astype(BF16)
    total = jnp.zeros((leaves, sizes["leaf_size"]), F32)
    for leaf in range(leaves):
        total += pick_row(leaf, jnp.dot(weights, left[cross_row:, columns_of(sizes, leaf)], preferred_element_type=F32))
    return total


def middle_kernel(
    sizes, near_index, partial, scales, own, packet, swapped, cross, blocks, left, slip, stress, halo
):
    picked = other_rows(sizes, near_index, own, swapped, cross)
    first = partial[...] + cross_part(sizes, scales, packet, swapped, left) + other_part(sizes, picked, blocks)
    halo[...] = (rows_of(slip, sizes["leaves"]) + jnp.tanh(first / 3.0)).astype(BF16)
    put_rows(stress, first)


def project_again(sizes, own, right, sums):
    total = jnp.zeros((sizes["leaves"], sizes["cross_rows"]), F32)
    for leaf in range(sizes["leaves"]):
        total += project_leaf(own[...], right[sizes["cross_row"] :, columns_of(sizes, leaf)], leaf)
    sums[...] = sums_row(total)


def ahead_again_kernel(sizes, ranks, own, blocks, right, left, partial, sums):
    @pl.when(early(sizes["ahead"]))
    def _():
        project_again(sizes, own, right, sums)

    @pl.when(ahead(sizes))
    def _():
        partial[...] = own_part(sizes, ranks, own, blocks, right, left)


def project_again_kernel(sizes, own, right, before, sums):
    done = early(sizes["ahead"])

    @pl.when(done)
    def _():
        sums[...] = before[...]

    @pl.when(jnp.logical_not(done))
    def _():
        project_again(sizes, own, right, sums)


def last_kernel(sizes, partial, scales, packet, swapped, left, first, first_stress, stress):
    first_stress[...] = first[...]
    put_rows(stress, partial[...] + cross_part(sizes, scales, packet, swapped, left))


def vmem(*arrays):
    return tuple(pltpu.with_memory_space_constraint(a, pltpu.VMEM) for a in arrays)


def hbm(*arrays):
    return tuple(pltpu.with_memory_space_constraint(a, pltpu.HBM) for a in arrays)


def local(slip_rate, near_blocks, near_index, far_left, far_right, far_ranks):
    leaves, near, leaf_size, _ = near_blocks.shape
    levels, rank, patches = far_left.shape
    local_levels = leaves.bit_length() - 1
    devices = lax.axis_size("leaf")
    chips = devices // 2
    local_rows = local_levels * rank
    cross_rows = levels * rank - local_rows
    sizes = dict(
        leaves=leaves, near=near, leaf_size=leaf_size, rank=rank, local_levels=local_levels,
        cross_levels=levels - local_levels, cross_row=local_rows, cross_rows=cross_rows, steps=2, ahead=2,
    )
    slip = slip_rate.reshape(-1, LANES)
    left = far_left.reshape(levels * rank, patches)
    right = far_right.reshape(levels * rank, patches)
    near_index = near_index.T
    shape = jax.ShapeDtypeStruct
    sums_shape = shape((1, cross_rows + -cross_rows % LANES), F32)
    partial_shape = shape((leaves, leaf_size), F32)
    stress_shape = shape(slip.shape, F32)
    swap = [(i, i ^ 1) for i in range(devices)]
    across = [(i, (i + 1) % devices) for i in range(1, devices, 2)]
    across += [(j, i) for i, j in across]
    order = sorted(range(chips), key=lambda chip: place_of(chip, chips))
    groups = [[chip * 2 + core for chip in order] for core in range(2)]

    def call(kernel, out_shape, specs, operands, mib=4, scratch=(), cost=None):
        outs = out_shape if isinstance(out_shape, tuple) else (out_shape,)
        return pl.pallas_call(
            lambda *refs: kernel(sizes, *refs),
            out_shape=out_shape,
            in_specs=specs,
            out_specs=tuple(VMEM_SPEC for _ in outs) if isinstance(out_shape, tuple) else VMEM_SPEC,
            scratch_shapes=scratch,
            compiler_params=pltpu.CompilerParams(vmem_limit_bytes=mib << 20),
            cost_estimate=cost,
        )(*operands)

    def permute(array, pairs):
        return lax.ppermute(array, "leaf", pairs)

    wait = pl.CostEstimate(flops=10**10, transcendentals=0, bytes_accessed=0)

    def exchange(sums, before, *rows):
        outgoing = call(
            spread_kernel, shape((chips, 1, LANES), F32), [VMEM_SPEC, ANY_SPEC], (sums, before), 1, cost=wait
        )
        incoming = lax.all_to_all(outgoing, "leaf", 0, 0, axis_index_groups=groups, tiled=True)
        packet = call(
            gather_kernel, shape((leaves + SUBLANES, leaf_size), F32) if rows else sums_shape,
            [VMEM_SPEC] * (2 + len(rows)), (sums, incoming, *rows), 1,
        )
        return packet

    kept = vmem(near_blocks, right, left)
    product_specs = [VMEM_SPEC] * 9

    halo_cross = permute(slip_rate, across).reshape(-1, LANES)
    project_scratch = [
        pltpu.VMEM(slip.shape, F32),
        pltpu.VMEM((cross_rows, patches), BF16),
        pltpu.SemaphoreType.DMA((sizes["steps"] + 1,)),
    ]
    sums, own = call(
        project_early_kernel, (sums_shape, partial_shape), [ANY_SPEC] * 2, hbm(slip, right),
        scratch=project_scratch,
    )
    before = call(
        own_ahead_kernel, partial_shape, [ANY_SPEC, VMEM_SPEC] + [ANY_SPEC] * 3,
        (*hbm(far_ranks), own, *hbm(near_blocks, right, left)), 8,
        [
            pltpu.VMEM(far_ranks.shape, jnp.int32),
            pltpu.VMEM((leaves, 1, leaf_size, leaf_size), BF16),
            pltpu.VMEM((local_rows, patches), BF16),
            pltpu.VMEM((local_rows, patches), BF16),
            pltpu.SemaphoreType.DMA((4,)),
        ],
    )
    sums, own = call(
        project_late_kernel, (sums_shape, partial_shape), [ANY_SPEC] * 2 + [VMEM_SPEC] * 2,
        (*hbm(slip, right), sums, own),
        scratch=project_scratch,
    )
    packet = exchange(sums, before, own)
    second, packet = call(
        own_second_kernel, (partial_shape, shape(packet.shape, F32)), [VMEM_SPEC] * 7,
        (far_ranks, own, *kept, before, packet),
    )
    swapped = permute(packet, swap)
    partial, scales = call(
        own_first_kernel, (partial_shape, shape((leaves, cross_rows), F32)), [VMEM_SPEC] * 7 + [ANY_SPEC],
        (far_ranks, own, *kept, before, second, packet),
    )
    first_stress, halo = call(
        middle_kernel, (pltpu.VMEM(slip.shape, F32), shape((leaves, leaf_size), BF16)), product_specs + [VMEM_SPEC],
        (near_index, partial, scales, own, packet, swapped, halo_cross, kept[0], kept[2], own),
    )
    halo_cross = permute(halo, across)
    halo_swap = permute(halo, swap)
    before, sums = call(ahead_again_kernel, (partial_shape, sums_shape), [VMEM_SPEC] * 5, (far_ranks, halo, *kept))
    sums = call(project_again_kernel, sums_shape, [VMEM_SPEC] * 3, (halo, kept[1], sums))
    packet = exchange(sums, before)
    swapped = permute(packet, swap)
    partial = call(
        near_kernel, partial_shape, [VMEM_SPEC] * 9 + [ANY_SPEC],
        (near_index, far_ranks, halo, halo_swap, halo_cross, *kept, before, packet),
    )
    first_stress, second_stress = call(
        last_kernel, (stress_shape, stress_shape), [VMEM_SPEC] * 6,
        (partial, scales, packet, swapped, kept[2], *vmem(first_stress)),
    )
    return (first_stress.reshape(-1), second_stress.reshape(-1))


def solution(mesh):
    in_specs = (
        P(("models", "leaf")),
        P(("models", "leaf"), None, None, None),
        P(("models", "leaf"), None),
        P(None, None, ("models", "leaf")),
        P(None, None, ("models", "leaf")),
        P(("models", "leaf"), None),
    )
    out_specs = (P(("models", "leaf")), P(("models", "leaf")))
    return jax.shard_map(local, mesh=mesh, in_specs=in_specs, out_specs=out_specs, check_vma=False)
```

```python
import math

import jax
import jax.numpy as jnp
from jax import lax
from jax.experimental import pallas as pl
from jax.experimental.pallas import tpu as pltpu
from jax.sharding import PartitionSpec as P


F32 = jnp.float32
BF16 = jnp.bfloat16
LANES = 128
SUBLANES = 8
VMEM_LIMIT = 67043328
RING = 32
NT = (((1,), (1,)), ((), ()))
TN = (((0,), (0,)), ((), ()))
VMEM_SPEC = pl.BlockSpec(memory_space=pltpu.VMEM)
ANY_SPEC = pl.BlockSpec(memory_space=pl.ANY)


def early(devices):
    return lax.axis_index("leaf") % RING < devices


def ahead(sizes):
    return jnp.logical_and(early(sizes["ahead"]), lax.axis_index("models") + lax.axis_index("leaf") > 0)


def sums_row(total):
    total = jnp.sum(total, axis=0, keepdims=True)
    pad = -total.shape[1] % LANES
    return jnp.concatenate([total, jnp.zeros((1, pad), F32)], axis=1) if pad else total


def rows_of(ref, leaves):
    if ref.shape[1] != LANES:
        return ref[:leaves, :]
    return jnp.concatenate([ref[pl.ds(0, leaves, stride=2), :], ref[pl.ds(1, leaves, stride=2), :]], axis=1)


def put_rows(flat, rows):
    leaves = rows.shape[0]
    flat[pl.ds(0, leaves, stride=2), :] = rows[:, :LANES]
    flat[pl.ds(1, leaves, stride=2), :] = rows[:, LANES:]


def columns_of(sizes, leaf):
    return slice(leaf * sizes["leaf_size"], (leaf + 1) * sizes["leaf_size"])


def pick_row(leaf, array):
    row = lax.broadcasted_iota(jnp.int32, array.shape, 0)
    return jnp.where(row == leaf, array, 0.0)


def project_leaf(rows, factor, leaf):
    return pick_row(leaf, lax.dot_general(rows, factor, NT, preferred_element_type=F32))


def project(sizes, slip_hbm, far_right, sums, own, slip, right_cross, sems):
    leaves, steps = sizes["leaves"], sizes["steps"]
    step = leaves // steps
    cross = pl.ds(sizes["cross_row"], sizes["cross_rows"])
    copies = [pltpu.make_async_copy(slip_hbm, slip, sems.at[steps])]
    for c in range(steps):
        columns = pl.ds(c * step * sizes["leaf_size"], step * sizes["leaf_size"])
        copies.append(pltpu.make_async_copy(far_right.at[cross, columns], right_cross.at[:, columns], sems.at[c]))
    for copy in copies:
        copy.start()
    copies[0].wait()
    own[...] = rows_of(slip, leaves)
    rows = own[...].astype(BF16)
    total = jnp.zeros((leaves, right_cross.shape[0]), F32)
    for leaf in range(leaves):
        if leaf % step == 0:
            copies[1 + leaf // step].wait()
        total += project_leaf(rows, right_cross[:, columns_of(sizes, leaf)], leaf)
    sums[...] = sums_row(total)


def early_kernel(
    sizes, slip_hbm, far_right, ranks_hbm, blocks_hbm, left_hbm, sums_hbm, own_hbm, partial_hbm,
    sums, own, partial, slip, right_cross, sems, ranks, blocks, right, left,
):
    steps = sizes["steps"]

    def put(values, target, number):
        copy = pltpu.make_async_copy(values, target, sems.at[steps + number])
        copy.start()
        return copy

    @pl.when(early(RING // 2))
    def _():
        project(sizes, slip_hbm, far_right, sums, own, slip, right_cross, sems)
        for copy in (put(sums, sums_hbm, 1), put(own, own_hbm, 2)):
            copy.wait()

    @pl.when(ahead(sizes))
    def _():
        copies = (
            put(far_right.at[pl.ds(0, right.shape[0])], right, 1),
            put(left_hbm.at[pl.ds(0, left.shape[0])], left, 2),
            put(blocks_hbm.at[:, pl.ds(0, 1)], blocks, 3),
            put(ranks_hbm, ranks, 4),
        )
        for copy in copies:
            copy.wait()
        partial[...] = own_part(sizes, ranks, own, blocks, right, left)
        put(partial, partial_hbm, 5).wait()


def late_kernel(sizes, *refs):
    @pl.when(jnp.logical_not(early(RING // 2)))
    def _():
        project(sizes, *refs)


def choose_kernel(sizes, early_sums, early_own, late_sums, late_own, sums, own):
    done = early(RING // 2)

    @pl.when(done)
    def _():
        sums[...] = early_sums[...]
        own[...] = early_own[...]

    @pl.when(jnp.logical_not(done))
    def _():
        sums[...] = late_sums[...]
        own[...] = late_own[...]


def place_of(chip, chips):
    return (chips - 1 - chips // 4 - chip) & (chips - 1)


def siblings(chip, chips, bit_no):
    start = (chip >> bit_no ^ 1) << bit_no
    return [place_of(start + step, chips) for step in range(2**bit_no)]


def lane_of(sizes, bit_no):
    return sizes["rank"] * (bit_no + 1)


def spread_kernel(sizes, own, _, outgoing):
    chip = lax.axis_index("leaf") // 2
    chips = outgoing.shape[0]
    total = own[...]
    outgoing[place_of(chip, chips)] = total[:, :LANES]
    for bit_no in range(sizes["cross_levels"] - 1):
        tile = lane_of(sizes, bit_no) // LANES * LANES
        for place in siblings(chip, chips, bit_no):
            outgoing[place] = total[:, tile : tile + LANES]


def gather_kernel(sizes, own, incoming, *refs):
    leaves = sizes["leaves"]
    chip = lax.axis_index("leaf") // 2
    total = own[...]
    bit_of = lax.broadcasted_iota(jnp.int32, total.shape, 1) // sizes["rank"]
    for bit_no in range(sizes["cross_levels"] - 1):
        part = sum(incoming[place] for place in siblings(chip, incoming.shape[0], bit_no))
        total = jnp.where(bit_of == 1 + bit_no, jnp.concatenate([part] * (total.shape[1] // LANES), axis=1), total)
    *rows, packet = refs
    if rows:
        packet[:leaves, :] = rows_of(rows[0], leaves).astype(F32)
        total = jnp.broadcast_to(total, (SUBLANES, total.shape[1]))
    packet[packet.shape[0] - total.shape[0] :, :] = total


def far_scales(sizes, ranks, first_level, levels):
    rank, leaf_size = sizes["rank"], sizes["leaf_size"]
    shape = (sizes["leaves"], levels * rank)
    lane = lax.broadcasted_iota(jnp.int32, shape, 1)
    limit, scale = jnp.zeros(shape, jnp.int32), jnp.zeros(shape, F32)
    for number in range(levels):
        level = first_level + number
        here = lane // rank == number
        limit = jnp.where(here, ranks[:, level : level + 1], limit)
        scale = jnp.where(here, 1.0 / math.sqrt(leaf_size * 2**level), scale)
    return jnp.where(lane % rank < limit, scale, 0.0)


def own_part(sizes, ranks, own, blocks, right, left):
    leaves, local_levels, rank = sizes["leaves"], sizes["local_levels"], sizes["rank"]
    local_rows = local_levels * rank
    rows = rows_of(own, leaves).astype(BF16)
    sums = jnp.zeros((leaves, local_rows), F32)
    for leaf in range(leaves):
        sums += project_leaf(rows, right[:local_rows, columns_of(sizes, leaf)], leaf)
    total = jnp.zeros((leaves, sizes["leaf_size"]), F32)
    for leaf in range(leaves):
        total += project_leaf(rows, blocks[leaf, 0], leaf)
    row = lax.broadcasted_iota(jnp.int32, sums.shape, 0)
    level_of = lax.broadcasted_iota(jnp.int32, sums.shape, 1) // rank
    stacked = sums
    for level in range(local_levels):
        span = 2**level
        low = row // span % 2 == 0
        partner = jnp.where(low, pltpu.roll(sums, leaves - span, 0), pltpu.roll(sums, span, 0))
        stacked = jnp.where(level_of == level, partner, stacked)
        sums = sums + partner
    weights = (stacked * far_scales(sizes, ranks, 0, local_levels)).astype(BF16)
    for leaf in range(leaves):
        total += pick_row(
            leaf, jnp.dot(weights, left[:local_rows, columns_of(sizes, leaf)], preferred_element_type=F32)
        )
    return total


def other_rows(sizes, near_index, own, swap, cross):
    leaves, near = sizes["leaves"], sizes["near"]
    device = lax.axis_index("leaf")
    odd = jnp.full((leaves, sizes["leaf_size"]), device % 2) == 1
    own, swap, cross = (rows_of(ref, leaves).astype(BF16).astype(F32) for ref in (own, swap, cross))
    extended = jnp.concatenate([jnp.where(odd, swap, cross), own, jnp.where(odd, cross, swap)], axis=0).astype(BF16)
    place = near_index[...] - (device - 1) * leaves
    row = lax.broadcasted_iota(jnp.int32, (3 * leaves, leaves), 0)
    picked = jnp.concatenate([jnp.where(row == place[k : k + 1, :], 1.0, 0.0) for k in range(1, near)], axis=1)
    rows = lax.dot_general(picked.astype(BF16), extended, TN, preferred_element_type=F32).astype(BF16)
    return [rows[k * leaves : (k + 1) * leaves, :] for k in range(near - 1)]


def second_core():
    return lax.axis_index("leaf") % 2 == 1


def own_or_before(sizes, ranks, own, blocks, right, left, before, partial):
    done = ahead(sizes)

    @pl.when(done)
    def _():
        partial[...] = before[...]

    @pl.when(jnp.logical_not(done))
    def _():
        partial[...] = own_part(sizes, ranks, own, blocks, right, left)


def own_second_kernel(sizes, ranks, own, blocks, right, left, before, packet, partial, packet_out):
    packet_out[...] = packet[...]

    @pl.when(second_core())
    def _():
        own_or_before(sizes, ranks, own, blocks, right, left, before, partial)


def own_first_kernel(sizes, ranks, own, blocks, right, left, before, second, _, partial, scales):
    scales[...] = far_scales(sizes, ranks, sizes["local_levels"], sizes["cross_levels"])

    @pl.when(second_core())
    def _():
        partial[...] = second[...]

    @pl.when(jnp.logical_not(second_core()))
    def _():
        own_or_before(sizes, ranks, own, blocks, right, left, before, partial)


def other_part(sizes, picked, blocks):
    total = jnp.zeros((sizes["leaves"], sizes["leaf_size"]), F32)
    for k, rows in enumerate(picked):
        for leaf in range(sizes["leaves"]):
            total += project_leaf(rows, blocks[leaf, 1 + k], leaf)
    return total


def near_kernel(sizes, near_index, ranks, own, swap, cross, blocks, right, left, before, _, partial):
    picked = other_rows(sizes, near_index, own, swap, cross)
    own_or_before(sizes, ranks, own, blocks, right, left, before, partial)
    partial[...] += other_part(sizes, picked, blocks)


def cross_part(sizes, scales, packet, swapped, left):
    leaves, cross_row, width = sizes["leaves"], sizes["cross_row"], sizes["cross_rows"]
    sums, others = packet[packet.shape[0] - 1 :, :], swapped[swapped.shape[0] - 1 :, :]
    lane = lax.broadcasted_iota(jnp.int32, sums.shape, 1)
    sums = others + jnp.where(lane < sizes["rank"], 0.0, sums)
    weights = (jnp.broadcast_to(sums[:, :width], (leaves, width)) * scales[...]).astype(BF16)
    total = jnp.zeros((leaves, sizes["leaf_size"]), F32)
    for leaf in range(leaves):
        total += pick_row(leaf, jnp.dot(weights, left[cross_row:, columns_of(sizes, leaf)], preferred_element_type=F32))
    return total


def middle_kernel(
    sizes, near_index, partial, scales, own, packet, swapped, cross, blocks, left, slip, stress, halo
):
    picked = other_rows(sizes, near_index, own, swapped, cross)
    first = partial[...] + cross_part(sizes, scales, packet, swapped, left) + other_part(sizes, picked, blocks)
    halo[...] = (rows_of(slip, sizes["leaves"]) + jnp.tanh(first / 3.0)).astype(BF16)
    put_rows(stress, first)


def project_again(sizes, own, right, sums):
    total = jnp.zeros((sizes["leaves"], sizes["cross_rows"]), F32)
    for leaf in range(sizes["leaves"]):
        total += project_leaf(own[...], right[sizes["cross_row"] :, columns_of(sizes, leaf)], leaf)
    sums[...] = sums_row(total)


def ahead_again_kernel(sizes, ranks, own, blocks, right, left, partial, sums):
    @pl.when(early(sizes["ahead"]))
    def _():
        project_again(sizes, own, right, sums)

    @pl.when(ahead(sizes))
    def _():
        partial[...] = own_part(sizes, ranks, own, blocks, right, left)


def project_again_kernel(sizes, own, right, before, sums):
    done = early(sizes["ahead"])

    @pl.when(done)
    def _():
        sums[...] = before[...]

    @pl.when(jnp.logical_not(done))
    def _():
        project_again(sizes, own, right, sums)


def last_kernel(sizes, partial, scales, packet, swapped, left, first, first_stress, stress):
    first_stress[...] = first[...]
    put_rows(stress, partial[...] + cross_part(sizes, scales, packet, swapped, left))


def vmem(*arrays):
    return tuple(pltpu.with_memory_space_constraint(a, pltpu.VMEM) for a in arrays)


def hbm(*arrays):
    return tuple(pltpu.with_memory_space_constraint(a, pltpu.HBM) for a in arrays)


def local(slip_rate, near_blocks, near_index, far_left, far_right, far_ranks):
    leaves, near, leaf_size, _ = near_blocks.shape
    levels, rank, patches = far_left.shape
    local_levels = leaves.bit_length() - 1
    devices = lax.axis_size("leaf")
    chips = devices // 2
    local_rows = local_levels * rank
    cross_rows = levels * rank - local_rows
    sizes = dict(
        leaves=leaves, near=near, leaf_size=leaf_size, rank=rank, local_levels=local_levels,
        cross_levels=levels - local_levels, cross_row=local_rows, cross_rows=cross_rows, steps=2, ahead=2,
    )
    slip = slip_rate.reshape(-1, LANES)
    left = far_left.reshape(levels * rank, patches)
    right = far_right.reshape(levels * rank, patches)
    near_index = near_index.T
    shape = jax.ShapeDtypeStruct
    sums_shape = shape((1, cross_rows + -cross_rows % LANES), F32)
    partial_shape = shape((leaves, leaf_size), F32)
    stress_shape = shape(slip.shape, F32)
    swap = [(i, i ^ 1) for i in range(devices)]
    across = [(i, (i + 1) % devices) for i in range(1, devices, 2)]
    across += [(j, i) for i, j in across]
    order = sorted(range(chips), key=lambda chip: place_of(chip, chips))
    groups = [[chip * 2 + core for chip in order] for core in range(2)]

    def call(kernel, out_shape, specs, operands, mib=4, scratch=(), cost=None, out_spec=VMEM_SPEC):
        outs = out_shape if isinstance(out_shape, tuple) else (out_shape,)
        return pl.pallas_call(
            lambda *refs: kernel(sizes, *refs),
            out_shape=out_shape,
            in_specs=specs,
            out_specs=tuple(out_spec for _ in outs) if isinstance(out_shape, tuple) else out_spec,
            scratch_shapes=scratch,
            compiler_params=pltpu.CompilerParams(vmem_limit_bytes=min(mib << 20, VMEM_LIMIT)),
            cost_estimate=cost,
        )(*operands)

    def permute(array, pairs):
        return lax.ppermute(array, "leaf", pairs)

    wait = pl.CostEstimate(flops=10**10, transcendentals=0, bytes_accessed=0)

    def exchange(sums, before, *rows):
        outgoing = call(
            spread_kernel, shape((chips, 1, LANES), F32), [VMEM_SPEC, ANY_SPEC], (sums, before), 1, cost=wait
        )
        incoming = lax.all_to_all(outgoing, "leaf", 0, 0, axis_index_groups=groups, tiled=True)
        packet = call(
            gather_kernel, shape((leaves + SUBLANES, leaf_size), F32) if rows else sums_shape,
            [VMEM_SPEC] * (2 + len(rows)), (sums, incoming, *rows), 1,
        )
        return packet

    kept = vmem(near_blocks, right, left)
    product_specs = [VMEM_SPEC] * 9

    halo_cross = permute(slip_rate, across).reshape(-1, LANES)
    project_scratch = [
        pltpu.VMEM(slip.shape, F32),
        pltpu.VMEM((cross_rows, patches), BF16),
        pltpu.SemaphoreType.DMA((sizes["steps"] + 1,)),
    ]
    *from_early, before = call(
        early_kernel, (sums_shape, partial_shape, partial_shape), [ANY_SPEC] * 5,
        hbm(slip, right, far_ranks, near_blocks, left), 64,
        [
            pltpu.VMEM(sums_shape.shape, F32),
            pltpu.VMEM(partial_shape.shape, F32),
            pltpu.VMEM(partial_shape.shape, F32),
            *project_scratch[:-1],
            pltpu.SemaphoreType.DMA((sizes["steps"] + 6,)),
            pltpu.VMEM(far_ranks.shape, jnp.int32),
            pltpu.VMEM((leaves, 1, leaf_size, leaf_size), BF16),
            pltpu.VMEM((local_rows, patches), BF16),
            pltpu.VMEM((local_rows, patches), BF16),
        ],
        out_spec=ANY_SPEC,
    )
    from_late = call(
        late_kernel, (sums_shape, partial_shape), [ANY_SPEC] * 2, hbm(slip, right), scratch=project_scratch
    )
    sums, own = call(choose_kernel, (sums_shape, partial_shape), [VMEM_SPEC] * 4, (*from_early, *from_late), 1)
    packet = exchange(sums, before, own)
    second, packet = call(
        own_second_kernel, (partial_shape, shape(packet.shape, F32)), [VMEM_SPEC] * 7,
        (far_ranks, own, *kept, before, packet),
    )
    swapped = permute(packet, swap)
    partial, scales = call(
        own_first_kernel, (partial_shape, shape((leaves, cross_rows), F32)), [VMEM_SPEC] * 7 + [ANY_SPEC],
        (far_ranks, own, *kept, before, second, packet),
    )
    first_stress, halo = call(
        middle_kernel, (pltpu.VMEM(slip.shape, F32), shape((leaves, leaf_size), BF16)), product_specs + [VMEM_SPEC],
        (near_index, partial, scales, own, packet, swapped, halo_cross, kept[0], kept[2], own),
    )
    halo_cross = permute(halo, across)
    halo_swap = permute(halo, swap)
    before, sums = call(ahead_again_kernel, (partial_shape, sums_shape), [VMEM_SPEC] * 5, (far_ranks, halo, *kept))
    sums = call(project_again_kernel, sums_shape, [VMEM_SPEC] * 3, (halo, kept[1], sums))
    packet = exchange(sums, before)
    swapped = permute(packet, swap)
    partial = call(
        near_kernel, partial_shape, [VMEM_SPEC] * 9 + [ANY_SPEC],
        (near_index, far_ranks, halo, halo_swap, halo_cross, *kept, before, packet),
    )
    first_stress, second_stress = call(
        last_kernel, (stress_shape, stress_shape), [VMEM_SPEC] * 6,
        (partial, scales, packet, swapped, kept[2], *vmem(first_stress)),
    )
    return (first_stress.reshape(-1), second_stress.reshape(-1))


def solution(mesh):
    in_specs = (
        P(("models", "leaf")),
        P(("models", "leaf"), None, None, None),
        P(("models", "leaf"), None),
        P(None, None, ("models", "leaf")),
        P(None, None, ("models", "leaf")),
        P(("models", "leaf"), None),
    )
    out_specs = (P(("models", "leaf")), P(("models", "leaf")))
    return jax.shard_map(local, mesh=mesh, in_specs=in_specs, out_specs=out_specs, check_vma=False)
```
